32 devices in a mesh: shard: 8 (over y, x, core), context: 2 (over z_hi), tensor: 2 (over z_lo).
Axes of the slice: x: 2, y: 2, z: 4 (z_hi: 2, z_lo: 2; z = z_hi * 2 + z_lo), core: 2. Of those that a mesh axis runs over, the one named last changes fastest.
Arguments:
- tokens: bfloat16 [8, 1024, 1536], P('shard', 'context'), may hold values from -6 to 6
- attention_gain: bfloat16 [1536], P('shard'), may hold values from 0.5 to 1.5
- query_weight: bfloat16 [1536, 1536], P('shard', 'tensor'), may hold values from -2 to 2
- key_matrix: bfloat16 [1536, 768], P('shard', 'tensor'), may hold values from -2 to 2
- value_matrix: bfloat16 [1536, 768], P('shard', 'tensor'), may hold values from -0.15625 to 0.15625
- output_weight: bfloat16 [1536, 1536], P('tensor', 'shard'), may hold values from -0.625 to 0.625
- feedforward_gain: bfloat16 [1536], P('shard'), may hold values from 0.5 to 1.5
- gate_weight: bfloat16 [1536, 4096], P('shard', 'tensor'), may hold values from -0.15625 to 0.15625
- up_weight: bfloat16 [1536, 4096], P('shard', 'tensor'), may hold values from -0.15625 to 0.15625
- down_weight: bfloat16 [4096, 1536], P('tensor', 'shard'), may hold values from -0.09375 to 0.09375
- cotangent: bfloat16 [8, 1024, 1536], P('shard', 'context'), may hold values from -6 to 6
Outputs:
- layer_output: bfloat16 [8, 1024, 1536], P('shard', 'context')
- input_grad: float32 [8, 1024, 1536], P('shard', 'context')
- attention_gain_grad: float32 [1536], P(('shard', 'context'))
- query_weight_grad: float32 [1536, 1536], P(('shard', 'context'), 'tensor')
- key_weight_grad: float32 [1536, 768], P(('shard', 'context'), 'tensor')
- value_weight_grad: float32 [1536, 768], P(('shard', 'context'), 'tensor')
- output_weight_grad: float32 [1536, 1536], P('tensor', ('shard', 'context'))
- feedforward_gain_grad: float32 [1536], P(('shard', 'context'))
- gate_weight_grad: float32 [1536, 4096], P(('shard', 'context'), 'tensor')
- up_weight_grad: float32 [1536, 4096], P(('shard', 'context'), 'tensor')
- down_weight_grad: float32 [4096, 1536], P('tensor', ('shard', 'context'))
The draws below stay inside these ranges and needn't reach their ends.
All inputs are finite; a program needn't handle non-finite values.
Results may differ from the reference program's by a relative error of at most 0.015.
Values may be sent and summed in bfloat16 or wider, within the bound.
A program may use at most 192 MiB of HBM per device.

```python
import math
import jax
import jax.numpy as jnp
from jax import lax

MODEL_WIDTH = 1536
QUERY_HEADS = 16
KEY_VALUE_HEADS = 8
HEAD_SIZE = 96
FF = 4096
SEQUENCE_LENGTH = 1024
SEQS = 8


def heads_scaled(key, columns):
    base = jax.random.truncated_normal(jax.random.fold_in(key, 11), -2.5, 2.5, (MODEL_WIDTH, columns), jnp.float32)
    base = base / jnp.sqrt(jnp.float32(MODEL_WIDTH))
    return base.astype(jnp.bfloat16)


def draw_query_weight(key, part):
    return heads_scaled(jax.random.fold_in(key, 1), QUERY_HEADS * HEAD_SIZE)


def draw_key_matrix(key, part):
    return heads_scaled(jax.random.fold_in(key, 2), KEY_VALUE_HEADS * HEAD_SIZE)


def with_spikes(array, key, source, target, blocks, factor):
    owner, partner = [(jnp.arange(array.shape[dim]) // (array.shape[dim] // blocks)).reshape([-1 if axis == dim else 1 for axis in range(array.ndim)]) for dim in (source, target)]
    chosen = jax.random.permutation(key, blocks)[partner]
    strong = (owner == chosen) | (owner == (partner + blocks // 2) % blocks)
    return jnp.where(strong, factor * array, array)


def block_levels(key, shape, shards, low, top_value):
    def one(position, shards_of):
        draws = jax.random.uniform(jax.random.fold_in(jax.random.fold_in(key, 6), position), (shards_of,), jnp.float32, low / len(shards), top_value / len(shards))
        return jnp.repeat(jnp.exp(draws), shape[position] // shards_of).reshape((-1,) + (1,) * (len(shape) - position - 1))

    level = one(*shards[0])
    for cut in shards[1:]:
        level = level * one(*cut)
    return level


def centred(key, shape, width, reach, cuts=(), kind=jnp.bfloat16):
    gain = block_levels(key, shape, cuts, -0.22, 0.18) if cuts else 1.0
    values = jax.random.normal(key, shape, jnp.float32) * width * gain
    return jnp.minimum(jnp.maximum(values, -reach), reach).astype(kind)


def bell_draw_with(rng, dims, width, limit, split, heavy, held_as=jnp.bfloat16):
    drawn = width * jax.random.normal(rng, dims, jnp.float32)
    if split:
        drawn = drawn * block_levels(rng, dims, split, -0.22, 0.18)
    return jnp.clip(with_spikes(drawn, jax.random.fold_in(rng, 3), *heavy), -limit, limit).astype(held_as)


def setup_inputs(seed: int = 0) -> dict:
    arg_keys = jax.random.split(jax.random.key(seed), 12)
    return {
        "tokens": centred(arg_keys[0], (SEQS, SEQUENCE_LENGTH, MODEL_WIDTH), 1.0, 6.0, ((0, 8), (1, 2))),
        "attention_gain": jnp.clip(1.0 + 0.1 * jax.random.normal(arg_keys[1], (MODEL_WIDTH,), jnp.float32), 0.5, 1.5).astype(jnp.bfloat16),
        "query_weight": draw_query_weight(jax.random.fold_in(arg_keys[11], 71), 0),
        "key_matrix": draw_key_matrix(jax.random.fold_in(arg_keys[11], 71), 0),
        "value_matrix": centred(arg_keys[4], (MODEL_WIDTH, KEY_VALUE_HEADS * HEAD_SIZE), MODEL_WIDTH ** -0.5, 0.15625, ((0, 8), (1, 2))),
        "output_weight": centred(arg_keys[5], (QUERY_HEADS * HEAD_SIZE, MODEL_WIDTH), (QUERY_HEADS * HEAD_SIZE // 16) ** -0.5, 0.625, ((0, 2), (1, 8))),
        "feedforward_gain": jnp.clip(1.0 + 0.1 * jax.random.normal(arg_keys[6], (MODEL_WIDTH,), jnp.float32), 0.5, 1.5).astype(jnp.bfloat16),
        "gate_weight": centred(arg_keys[7], (MODEL_WIDTH, FF), MODEL_WIDTH ** -0.5, 0.15625, ((0, 8), (1, 2))),
        "up_weight": centred(arg_keys[8], (MODEL_WIDTH, FF), MODEL_WIDTH ** -0.5, 0.15625, ((0, 8), (1, 2))),
        "down_weight": centred(arg_keys[9], (FF, MODEL_WIDTH), FF ** -0.5, 0.09375, ((0, 2), (1, 8))),
        "cotangent": bell_draw_with(arg_keys[10], (SEQS, SEQUENCE_LENGTH, MODEL_WIDTH), 1.0, 6.0, ((0, 8), (1, 2)), (0, 2, 8, 2.0)),
    }


EPS = 1e-05
THETA = 100000.0
PRECISE_MODE = lax.Precision.HIGHEST

@jax.custom_vjp
def lowered_precision(v):
    return lax.optimization_barrier(v.astype(jnp.bfloat16)).astype(jnp.float32)

@jax.custom_vjp
def lowered_backward(v):
    return v

def low_keep(v):
    return (lowered_precision(v), None)

def low_pass(kept, grad):
    return (grad,)

def back_keep(v):
    return (v, None)

def back_low(kept, grad):
    return (lowered_precision(grad),)
lowered_precision.defvjp(low_keep, low_pass)
lowered_backward.defvjp(back_keep, back_low)

def rotation(positions):
    half_dim = HEAD_SIZE // 2
    spin_rates = THETA ** (-jnp.arange(half_dim, dtype=jnp.float32) * 2.0 / HEAD_SIZE)
    angles = positions.astype(jnp.float32)[:, None] * spin_rates[None, :]
    angles = jnp.concatenate([angles, angles], axis=-1)
    return (jnp.cos(angles), jnp.sin(angles))

def rotate(value_rows, cosine, sine_part):
    half_dim = HEAD_SIZE // 2
    turned = jnp.concatenate([-value_rows[..., half_dim:], value_rows[..., :half_dim]], axis=-1)
    return value_rows * cosine + turned * sine_part

def attend_block(block_of_queries, start, key_rows, value_rows):
    batch_inputs = block_of_queries.shape[0]
    rows_per_block = block_of_queries.shape[1]
    grouped_heads = block_of_queries.reshape(batch_inputs, rows_per_block, KEY_VALUE_HEADS, QUERY_HEADS // KEY_VALUE_HEADS, HEAD_SIZE)
    scores = jnp.einsum('bqkgd,blkd->bkgql', grouped_heads, key_rows, precision=PRECISE_MODE) * HEAD_SIZE ** (-0.5)
    scores = lowered_backward(scores)
    row_index = start + jnp.arange(rows_per_block, dtype=jnp.int32)
    columns = jnp.arange(SEQUENCE_LENGTH, dtype=jnp.int32)
    scores = jnp.where(columns[None, :] <= row_index[:, None], scores, -jnp.inf)
    peak = lax.optimization_barrier(jnp.max(scores, axis=-1, keepdims=True))
    weights = jnp.exp(scores - peak)
    probabilities = weights / lax.optimization_barrier(jnp.sum(weights, axis=-1, keepdims=True))
    mixed = jnp.einsum('bkgql,blkd->bqkgd', lowered_precision(probabilities), value_rows, precision=PRECISE_MODE)
    return mixed.reshape(batch_inputs, rows_per_block, QUERY_HEADS, HEAD_SIZE)

def layer(tokens, attention_gain, query_weight, key_matrix, value_matrix, output_weight, feedforward_gain, gate_weight, up_weight, down_weight):
    batch_inputs = tokens.shape[0]
    flat = tokens.reshape(batch_inputs * SEQUENCE_LENGTH, MODEL_WIDTH)
    first_normed = lowered_precision(flat * lax.rsqrt(lax.optimization_barrier(jnp.mean(flat * flat, axis=-1, keepdims=True)) + EPS) * attention_gain)
    cosine, sine_part = rotation(jnp.arange(SEQUENCE_LENGTH, dtype=jnp.int32))
    cosine = cosine[None, :, None, :]
    sine_part = sine_part[None, :, None, :]
    query = lowered_backward(jnp.dot(first_normed, query_weight, precision=PRECISE_MODE)).reshape(batch_inputs, SEQUENCE_LENGTH, QUERY_HEADS, HEAD_SIZE)
    query = lowered_precision(rotate(query, cosine, sine_part))
    key_rows = lowered_backward(jnp.dot(first_normed, key_matrix, precision=PRECISE_MODE)).reshape(batch_inputs, SEQUENCE_LENGTH, KEY_VALUE_HEADS, HEAD_SIZE)
    key_rows = lowered_precision(rotate(key_rows, cosine, sine_part))
    value_rows = lowered_precision(lowered_backward(jnp.dot(first_normed, value_matrix, precision=PRECISE_MODE))).reshape(batch_inputs, SEQUENCE_LENGTH, KEY_VALUE_HEADS, HEAD_SIZE)
    rows_per_block = min(512, SEQUENCE_LENGTH)
    count = SEQUENCE_LENGTH // rows_per_block
    pieces = query.reshape(batch_inputs, count, rows_per_block, QUERY_HEADS, HEAD_SIZE).transpose(1, 0, 2, 3, 4)
    starts = jnp.arange(count, dtype=jnp.int32) * rows_per_block
    checked = jax.checkpoint(attend_block)
    mixed = lax.map(lambda pair: checked(pair[0], pair[1], key_rows, value_rows), (pieces, starts))
    attended = mixed.transpose(1, 0, 2, 3, 4).reshape(batch_inputs * SEQUENCE_LENGTH, QUERY_HEADS * HEAD_SIZE)
    attended = lowered_precision(lowered_backward(attended))
    middle = flat + lowered_backward(jnp.dot(attended, output_weight, precision=PRECISE_MODE))
    normed_two = lowered_precision(middle * lax.rsqrt(lax.optimization_barrier(jnp.mean(middle * middle, axis=-1, keepdims=True)) + EPS) * feedforward_gain)
    gate = lowered_backward(jnp.dot(normed_two, gate_weight, precision=PRECISE_MODE))
    upward = lowered_backward(jnp.dot(normed_two, up_weight, precision=PRECISE_MODE))
    hidden = lowered_precision(gate * jax.nn.sigmoid(gate) * upward)
    result = middle + jnp.dot(hidden, down_weight, precision=PRECISE_MODE)
    return result.reshape(batch_inputs, SEQUENCE_LENGTH, MODEL_WIDTH)

def reference(tokens, attention_gain, query_weight, key_matrix, value_matrix, output_weight, feedforward_gain, gate_weight, up_weight, down_weight, cotangent):
    weights = tuple((item.astype(jnp.float32) for item in (attention_gain, query_weight, key_matrix, value_matrix, output_weight, feedforward_gain, gate_weight, up_weight, down_weight)))
    group = math.gcd(SEQS, max(1, 4096 // SEQUENCE_LENGTH))
    inputs = tokens.astype(jnp.float32).reshape(SEQS // group, group, SEQUENCE_LENGTH, MODEL_WIDTH)
    pulls = cotangent.astype(jnp.float32).reshape(SEQS // group, group, SEQUENCE_LENGTH, MODEL_WIDTH)

    def step(totals, pair):
        inside, pulled = pair
        result, backward = jax.vjp(layer, inside, *weights)
        grads = backward(pulled)
        totals = tuple((total + grad for total, grad in zip(totals, grads[1:])))
        return (totals, (result.astype(jnp.bfloat16), grads[0]))
    zeros = tuple((jnp.zeros(item.shape, jnp.float32) for item in weights))
    totals, (results, input_grads) = lax.scan(step, zeros, (inputs, pulls))
    return (results.reshape(SEQS, SEQUENCE_LENGTH, MODEL_WIDTH), input_grads.reshape(SEQS, SEQUENCE_LENGTH, MODEL_WIDTH), totals[0], totals[1], totals[2], totals[3], totals[4], totals[5], totals[6], totals[7], totals[8])
```

```python
import jax
import jax.numpy as jnp
from jax import lax
from jax.sharding import PartitionSpec as P

HEAD_SIZE = 96
EPS = 1e-05
THETA = 100000.0
BF16 = jnp.bfloat16
F32 = jnp.float32


def rotation(positions):
    half_dim = HEAD_SIZE // 2
    spin_rates = THETA ** (-jnp.arange(half_dim, dtype=F32) * 2.0 / HEAD_SIZE)
    angles = positions.astype(F32)[:, None] * spin_rates[None, :]
    angles = jnp.concatenate([angles, angles], axis=-1)
    return (jnp.cos(angles), jnp.sin(angles))


def rotate(value_rows, cosine, sine_part):
    half_dim = HEAD_SIZE // 2
    turned = jnp.concatenate([-value_rows[..., half_dim:], value_rows[..., :half_dim]], axis=-1)
    return value_rows * cosine + turned * sine_part


def unrotate(grads, cosine, sine_part):
    half_dim = HEAD_SIZE // 2
    moved = grads * sine_part
    back_turn = jnp.concatenate([moved[..., half_dim:], -moved[..., :half_dim]], axis=-1)
    return grads * cosine + back_turn


def norm_rows(flat, gain):
    inverse = lax.rsqrt(jnp.mean(flat * flat, axis=-1, keepdims=True) + EPS)
    plain = flat * inverse
    return (plain, inverse, (plain * gain).astype(BF16))


def norm_back(normed_grad, plain, inverse, gain):
    weighted = normed_grad * gain
    inner = jnp.mean(weighted * plain, axis=-1, keepdims=True)
    return inverse * (weighted - plain * inner)


def dot(left, right):
    return jnp.dot(left, right, preferred_element_type=F32)


def rows_dot(left, right):
    return lax.dot_general(left, right, (((0,), (0,)), ((), ())), preferred_element_type=F32)


def dot_t(left, right):
    return lax.dot_general(left, right, (((1,), (1,)), ((), ())), preferred_element_type=F32)


class Plane:
    def __init__(self, width):
        self.count = lax.axis_size("shard")
        self.chips = self.count // 2
        self.me = lax.axis_index("shard")
        self.rows = width // self.count
        self.half = width // 2

    def order(self, me):
        return [
            ((me // 2) ^ chip) * 2 + ((me % 2) ^ core)
            for core in range(2)
            for chip in range(self.chips)
        ]

    def relative(self, array):
        def branch(me):
            return lambda a: jnp.concatenate(
                [a[:, g * self.rows : (g + 1) * self.rows] for g in self.order(me)], axis=1
            )

        return lax.switch(self.me, [branch(me) for me in range(self.count)], array)

    def absolute(self, array):
        def branch(me):
            order = self.order(me)
            return lambda a: jnp.concatenate(
                [
                    a[:, order.index(g) * self.rows : (order.index(g) + 1) * self.rows]
                    for g in range(self.count)
                ],
                axis=1,
            )

        return lax.switch(self.me, [branch(me) for me in range(self.count)], array)

    def to_chip(self, array, chip):
        return lax.ppermute(array, "shard", [(i, i ^ (2 * chip)) for i in range(self.count)])

    def to_core(self, array):
        return lax.ppermute(array, "shard", [(i, i ^ 1) for i in range(self.count)])

    def gather(self, array, axis=0):
        parts = [array] + [self.to_chip(array, chip) for chip in range(1, self.chips)]
        near = jnp.concatenate(parts, axis=axis)
        return near, self.to_core(near)

    def pair(self, left, right):
        return (left[:, : self.half], right, self.to_core(left[:, self.half :]), self.to_core(right))

    def weight_grad(self, paired):
        left, right, left_other, right_other = paired
        total = None
        for chip in reversed(range(self.chips)):
            cols = slice(chip * self.rows, (chip + 1) * self.rows)
            part = rows_dot(left[:, cols], right) + rows_dot(left_other[:, cols], right_other)
            if chip:
                part = self.to_chip(part.astype(BF16), chip).astype(F32)
            total = part if total is None else total + part
        return context_half(total)

    def gain_grads(self, stacked):
        other = self.to_core(stacked[:, self.half :])
        stacked = stacked[:, : self.half] + other
        total = stacked[:, : self.rows]
        for chip in range(1, self.chips):
            total = total + self.to_chip(
                stacked[:, chip * self.rows : (chip + 1) * self.rows], chip
            )
        half = self.rows // 2
        own = lax.axis_index("context")
        keep = lax.dynamic_slice_in_dim(total, own * half, half, 1)
        send = lax.dynamic_slice_in_dim(total, (1 - own) * half, half, 1)
        return keep + over_context(send)


def over_context(array):
    return lax.ppermute(array, "context", [(0, 1), (1, 0)])


def over_tensor(array):
    return lax.ppermute(array, "tensor", [(0, 1), (1, 0)])


def context_half(total):
    half = total.shape[0] // 2
    own = lax.axis_index("context")
    keep = lax.dynamic_slice_in_dim(total, own * half, half, 0)
    send = lax.dynamic_slice_in_dim(total, (1 - own) * half, half, 0)
    return keep + over_context(send.astype(BF16)).astype(F32)


def tensor_sum(part):
    return part + over_tensor(part.astype(BF16)).astype(F32)


def score_parts(grouped, keys, factor):
    rows = grouped.shape[0]
    own_context = lax.axis_index("context")
    scores = (
        jnp.einsum("qkgd,lkd->kgql", grouped, keys, preferred_element_type=F32) * factor
    )
    row_index = jnp.arange(rows)[:, None] + rows
    columns = jnp.arange(keys.shape[0])[None, :]
    first = jnp.where(own_context == 0, rows, 0)
    return jnp.where((columns <= row_index) & (columns >= first), scores, -jnp.inf)


def shards(
    tokens,
    attention_gain,
    query_weight,
    key_matrix,
    value_matrix,
    output_weight,
    feedforward_gain,
    gate_weight,
    up_weight,
    down_weight,
    cotangent,
):
    width = tokens.shape[-1]
    rows_local = tokens.shape[0] * tokens.shape[1]
    plane = Plane(width)
    half = plane.half
    own_context = lax.axis_index("context")
    query_cols = query_weight.shape[1]
    value_cols = key_matrix.shape[1]
    heads_query = query_cols // HEAD_SIZE
    heads_value = value_cols // HEAD_SIZE
    group = heads_query // heads_value
    factor = HEAD_SIZE ** (-0.5)

    gains = jnp.concatenate(
        plane.gather(jnp.stack([attention_gain, feedforward_gain]), axis=1), axis=1
    ).astype(F32)
    gain_one, gain_two = gains[0:1], gains[1:2]
    proj_a, proj_b = plane.gather(jnp.concatenate([query_weight, key_matrix, value_matrix], axis=1))
    out_a, out_b = plane.gather(output_weight.T)
    gate_a, gate_b = plane.gather(gate_weight)
    up_a, up_b = plane.gather(up_weight)
    down_a, down_b = plane.gather(down_weight.T)

    flat = plane.relative(tokens.reshape(rows_local, width)).astype(F32)
    grad_out = plane.relative(cotangent.reshape(rows_local, width))
    plain_one, inverse_one, first_normed = norm_rows(flat, gain_one)
    cosine, sine_part = rotation(own_context * rows_local + jnp.arange(rows_local))
    cosine, sine_part = cosine[:, None, :], sine_part[:, None, :]

    proj = dot(first_normed[:, :half], proj_a) + dot(first_normed[:, half:], proj_b)
    rotated = rotate(
        proj[:, : query_cols + value_cols].reshape(rows_local, -1, HEAD_SIZE), cosine, sine_part
    ).astype(BF16)
    query = rotated[:, :heads_query].reshape(rows_local, heads_value, group, HEAD_SIZE)
    key = rotated[:, heads_query:]
    value = proj[:, query_cols + value_cols :].astype(BF16)
    packed = jnp.concatenate([key.reshape(rows_local, value_cols), value], axis=1)
    earlier = lax.ppermute(packed, "context", [(0, 1)])
    keys = jnp.concatenate([earlier[:, :value_cols], packed[:, :value_cols]]).reshape(
        -1, heads_value, HEAD_SIZE
    )
    values = jnp.concatenate([earlier[:, value_cols:], packed[:, value_cols:]]).reshape(
        -1, heads_value, HEAD_SIZE
    )
    scores = score_parts(query, keys, factor)
    peak = jnp.max(scores, axis=-1, keepdims=True)
    weights = jnp.exp(scores - peak)
    total = jnp.sum(weights, axis=-1, keepdims=True)
    attended = (
        jnp.einsum(
            "kgql,lkd->qkgd", (weights / total).astype(BF16), values, preferred_element_type=F32
        )
        .astype(BF16)
        .reshape(rows_local, query_cols)
    )
    lse = peak + jnp.log(total)
    branch = jnp.concatenate([dot_t(attended, out_a), dot_t(attended, out_b)], axis=1)
    middle = flat + tensor_sum(branch)

    plain_two, inverse_two, normed_two = norm_rows(middle, gain_two)
    near, far = normed_two[:, :half], normed_two[:, half:]
    gate_value = dot(near, gate_a) + dot(far, gate_b)
    up_value = dot(near, up_a) + dot(far, up_b)
    sigma = jax.nn.sigmoid(gate_value)
    swish = gate_value * sigma
    hidden = (swish * up_value).astype(BF16)
    hidden_grad = dot(grad_out[:, :half], down_a) + dot(grad_out[:, half:], down_b)
    grad_gate = (hidden_grad * up_value * sigma * (1.0 + gate_value * (1.0 - sigma))).astype(BF16)
    grad_up = (hidden_grad * swish).astype(BF16)
    normed_grad = jnp.concatenate(
        [
            dot_t(grad_gate, gate_a) + dot_t(grad_up, up_a),
            dot_t(grad_gate, gate_b) + dot_t(grad_up, up_b),
        ],
        axis=1,
    )
    normed_grad = tensor_sum(normed_grad)
    mixed = jnp.concatenate([dot_t(hidden, down_a), dot_t(hidden, down_b)], axis=1)
    result = middle + tensor_sum(mixed)
    layer_output = plane.absolute(result.astype(BF16)).reshape(tokens.shape)

    gate_pair = plane.pair(normed_two, grad_gate)
    gate_weight_grad = plane.weight_grad(gate_pair)
    up_other = plane.to_core(grad_up)
    up_weight_grad = plane.weight_grad((gate_pair[0], grad_up, gate_pair[2], up_other))
    down_weight_grad = plane.weight_grad(plane.pair(grad_out, hidden)).T

    middle_grad = norm_back(normed_grad, plain_two, inverse_two, gain_two) + grad_out.astype(F32)
    branch_low = middle_grad.astype(BF16)
    attended_grad = (
        (dot(branch_low[:, :half], out_a) + dot(branch_low[:, half:], out_b))
        .astype(BF16)
        .reshape(rows_local, heads_value, group, HEAD_SIZE)
    )
    output_weight_grad = plane.weight_grad(plane.pair(branch_low, attended)).T

    scores = score_parts(query, keys, factor)
    probs = jnp.exp(scores - lse)
    prob_grad = jnp.einsum("qkgd,lkd->kgql", attended_grad, values, preferred_element_type=F32)
    inner = jnp.sum(probs * prob_grad, axis=-1, keepdims=True)
    score_grad = (probs * (prob_grad - inner)).astype(BF16)
    query_back = (
        jnp.einsum("kgql,lkd->qkgd", score_grad, keys, preferred_element_type=F32) * factor
    )
    key_back = jnp.einsum("kgql,qkgd->lkd", score_grad, query, preferred_element_type=F32) * factor
    value_back = jnp.einsum(
        "kgql,qkgd->lkd", probs.astype(BF16), attended_grad, preferred_element_type=F32
    )
    sent = jnp.concatenate([key_back[:rows_local], value_back[:rows_local]], axis=1).astype(BF16)
    later = lax.ppermute(sent.reshape(rows_local, 2 * value_cols), "context", [(1, 0)])
    later = later.reshape(rows_local, 2 * heads_value, HEAD_SIZE).astype(F32)
    key_back = key_back[rows_local:] + later[:, :heads_value]
    value_back = value_back[rows_local:] + later[:, heads_value:]
    query_grad = unrotate(
        query_back.reshape(rows_local, heads_query, HEAD_SIZE), cosine, sine_part
    ).astype(BF16)
    key_grad = unrotate(key_back, cosine, sine_part).astype(BF16)
    proj_grad = jnp.concatenate([query_grad, key_grad, value_back.astype(BF16)], axis=1).reshape(
        rows_local, -1
    )
    normed_one_part = jnp.concatenate([dot_t(proj_grad, proj_a), dot_t(proj_grad, proj_b)], axis=1)
    normed_one_grad = tensor_sum(normed_one_part)
    proj_weight_grad = plane.weight_grad(plane.pair(first_normed, proj_grad))
    input_grad = middle_grad + norm_back(normed_one_grad, plain_one, inverse_one, gain_one)
    input_grad = plane.absolute(input_grad)
    gain_grads = plane.gain_grads(
        jnp.stack(
            [jnp.sum(normed_one_grad * plain_one, axis=0), jnp.sum(normed_grad * plain_two, axis=0)]
        )
    )
    return (
        layer_output,
        input_grad.reshape(tokens.shape),
        gain_grads[0],
        proj_weight_grad[:, :query_cols],
        proj_weight_grad[:, query_cols : query_cols + value_cols],
        proj_weight_grad[:, query_cols + value_cols :],
        output_weight_grad,
        gain_grads[1],
        gate_weight_grad,
        up_weight_grad,
        down_weight_grad,
    )


def solution(mesh):
    in_specs = (
        P("shard", "context", None),
        P("shard"),
        P("shard", "tensor"),
        P("shard", "tensor"),
        P("shard", "tensor"),
        P("tensor", "shard"),
        P("shard"),
        P("shard", "tensor"),
        P("shard", "tensor"),
        P("tensor", "shard"),
        P("shard", "context", None),
    )
    out_specs = (
        P("shard", "context", None),
        P("shard", "context", None),
        P(("shard", "context")),
        P(("shard", "context"), "tensor"),
        P(("shard", "context"), "tensor"),
        P(("shard", "context"), "tensor"),
        P("tensor", ("shard", "context")),
        P(("shard", "context")),
        P(("shard", "context"), "tensor"),
        P(("shard", "context"), "tensor"),
        P("tensor", ("shard", "context")),
    )
    return jax.shard_map(shards, mesh=mesh, in_specs=in_specs, out_specs=out_specs, check_vma=False)
```

```python
import functools

import jax
import jax.numpy as jnp
from jax import lax
from jax.experimental import pallas as pl
from jax.experimental.pallas import tpu as pltpu
from jax.sharding import PartitionSpec as P

HEAD_SIZE = 96
EPS = 1e-05
THETA = 100000.0
BF16 = jnp.bfloat16
F32 = jnp.float32
NEG = -1e30
LANES = 128


VMEM = pl.BlockSpec(memory_space=pltpu.VMEM)
SMEM = pl.BlockSpec(memory_space=pltpu.SMEM)


def shape(rows, cols, kind=BF16):
    return jax.ShapeDtypeStruct((rows, cols), kind)


def cost(flops, moved):
    return pl.CostEstimate(flops=int(flops), bytes_accessed=int(moved), transcendentals=0)


def rotation(positions):
    half_dim = HEAD_SIZE // 2
    spin_rates = THETA ** (-jnp.arange(half_dim, dtype=F32) * 2.0 / HEAD_SIZE)
    angles = positions.astype(F32)[:, None] * spin_rates[None, :]
    angles = jnp.concatenate([angles, angles], axis=-1)
    return (jnp.cos(angles), jnp.sin(angles))


def dot_nn(a, b):
    return lax.dot_general(a, b, (((1,), (0,)), ((), ())), preferred_element_type=F32)


def dot_nt(a, b):
    return lax.dot_general(a, b, (((1,), (1,)), ((), ())), preferred_element_type=F32)


def flip(a):
    return a.astype(F32).T.astype(a.dtype)


def rotate(v, cosine, sine_part):
    half_dim = HEAD_SIZE // 2
    turned = jnp.concatenate([-v[:, half_dim:], v[:, :half_dim]], axis=1)
    return v * cosine + turned * sine_part


def unrotate(u, cosine, sine_part):
    half_dim = HEAD_SIZE // 2
    s = u * sine_part
    return u * cosine + jnp.concatenate([s[:, half_dim:], -s[:, :half_dim]], axis=1)


def causal(scores, first):
    keys = lax.broadcasted_iota(jnp.int32, scores.shape, 0)
    queries = lax.broadcasted_iota(jnp.int32, scores.shape, 1)
    return jnp.where(keys <= queries + first, scores, NEG)


def inverse_rms(x):
    return lax.rsqrt(jnp.mean(x * x, axis=-1, keepdims=True) + EPS)


def exchange_blocks(x, me, rows, chips):
    width = x.shape[1]
    step, bit = width // 2, me % 2
    while True:
        parts = []
        for first in range(0, width, 2 * step):
            parts += [x[:, first + step : first + 2 * step], x[:, first : first + step]]
        x = jnp.where(bit > 0, jnp.concatenate(parts, axis=1), x)
        step //= 2
        if step < rows:
            return x
        bit = (me // 2) // (step // rows) % 2


def to_relative(x, me, rows, chips):
    blocks = [
        x[:, (chip * 2 + core) * rows : (chip * 2 + core + 1) * rows]
        for core in range(2)
        for chip in range(chips)
    ]
    return exchange_blocks(jnp.concatenate(blocks, axis=1), me, rows, chips)


def to_absolute(x, me, rows, chips):
    x = exchange_blocks(x, me, rows, chips)
    blocks = [
        x[:, (core * chips + chip) * rows : (core * chips + chip + 1) * rows]
        for chip in range(chips)
        for core in range(2)
    ]
    return jnp.concatenate(blocks, axis=1)


def row_loop(total, body, step=64):
    def one(i, carry):
        body(pl.ds(pl.multiple_of(i * step, step), step))
        return carry

    lax.fori_loop(0, total // step, one, 0)


def enter_kernel(rows, chips, me_ref, tokens_ref, low_ref, high_ref):
    half = low_ref.shape[1]

    def body(at):
        x = to_relative(tokens_ref[at, :].astype(F32), me_ref[0], rows, chips).astype(BF16)
        low_ref[at, :] = x[:, :half]
        high_ref[at, :] = x[:, half:]

    row_loop(tokens_ref.shape[0], body)


def enter(me, tokens, rows, chips):
    count, width = tokens.shape
    return pl.pallas_call(
        functools.partial(enter_kernel, rows, chips),
        out_shape=(shape(count, width // 2),) * 2,
        in_specs=[SMEM, VMEM],
        out_specs=(VMEM,) * 2,
        cost_estimate=cost(0, 6 * count * width),
        name="enter",
    )(me, tokens)


def leave_kernel(rows, chips, me_ref, middle_ref, own_ref, other_ref, out_ref):
    def body(at):
        x = middle_ref[at, :] + (own_ref[at, :].astype(F32) + other_ref[at, :].astype(F32))
        out_ref[at, :] = to_absolute(x, me_ref[0], rows, chips).astype(BF16)

    row_loop(own_ref.shape[0], body)


def leave(me, middle, own, other, rows, chips):
    return pl.pallas_call(
        functools.partial(leave_kernel, rows, chips),
        out_shape=shape(*own.shape),
        in_specs=[SMEM] + [VMEM] * 3,
        out_specs=VMEM,
        cost_estimate=cost(0, 8 * own.size),
        name="leave",
    )(me, middle, own, other)


def finish_kernel(rows, chips, me_ref, own_ref, other_ref, grad_ref, low_ref, high_ref, gain_ref, out_ref):
    gain = gain_ref[0:1, :]

    def body(at):
        x = jnp.concatenate([low_ref[at, :], high_ref[at, :]], axis=1).astype(F32)
        inverse = inverse_rms(x)
        plain = x * inverse
        weighted = (own_ref[at, :].astype(F32) + other_ref[at, :].astype(F32)) * gain
        inner = jnp.mean(weighted * plain, axis=-1, keepdims=True)
        grad = grad_ref[at, :] + inverse * (weighted - plain * inner)
        out_ref[at, :] = to_absolute(grad, me_ref[0], rows, chips)

    row_loop(own_ref.shape[0], body)


def finish(me, own, other, grad, low, high, gains, rows, chips):
    return pl.pallas_call(
        functools.partial(finish_kernel, rows, chips),
        out_shape=shape(*own.shape, F32),
        in_specs=[SMEM] + [VMEM] * 6,
        out_specs=VMEM,
        cost_estimate=cost(0, 16 * own.size),
        name="finish",
    )(me, own, other, grad, low, high, gains)


def attend_kernel(
    heads, group, tile, place_ref, low_ref, high_ref, piece_ref, rest_ref, near_ref, far_ref,
    cos_ref, sin_ref, cos0_ref, sin0_ref,
    normed_low_ref, normed_high_ref, attended_ref, query_ref, key_ref, value_ref, key0_ref, value0_ref,
    lse_ref, gain_ref, branch_ref, proj_ref, early_ref,
):
    factor = HEAD_SIZE ** (-0.5)
    rows, half = low_ref.shape
    query_cols = heads * group * HEAD_SIZE
    key_cols = heads * HEAD_SIZE
    proj_cols = query_cols + 2 * key_cols
    out_cols = slice(proj_cols, proj_cols + query_cols)
    gain_cols = slice(proj_cols + query_cols, proj_cols + query_cols + LANES)
    gains = jnp.concatenate(
        [near_ref[:, gain_cols].astype(F32).T[0:2], far_ref[:, gain_cols].astype(F32).T[0:2]], axis=1
    )
    gain_ref[...] = gains
    gain = gains[0:1]

    def normed(low, high):
        x = jnp.concatenate([low, high], axis=1).astype(F32)
        x = (x * inverse_rms(x) * gain).astype(BF16)
        return x[:, :half], x[:, half:]

    low, high = normed(low_ref[...], high_ref[...])
    normed_low_ref[...] = low
    normed_high_ref[...] = high
    proj_ref[...] = dot_nn(low, near_ref[:, :proj_cols]) + dot_nn(high, far_ref[:, :proj_cols])
    first_piece = place_ref[1] == 0
    piece, rest = piece_ref[...].astype(F32), rest_ref[...].astype(F32)
    low, high = normed(jnp.where(first_piece, piece, rest), jnp.where(first_piece, rest, piece))
    early_ref[...] = dot_nn(low, near_ref[:, query_cols:proj_cols]) + dot_nn(
        high, far_ref[:, query_cols:proj_cols]
    )
    bias = jnp.where(place_ref[0] > 0, 0.0, NEG).astype(F32)
    cosine, sine_part, cosine0, sine0 = cos_ref[...], sin_ref[...], cos0_ref[...], sin0_ref[...]
    for j in range(heads):
        cols = slice(j * HEAD_SIZE, (j + 1) * HEAD_SIZE)
        start = query_cols + j * HEAD_SIZE
        key = rotate(proj_ref[:, start : start + HEAD_SIZE], cosine, sine_part).astype(BF16)
        start += key_cols
        value = proj_ref[:, start : start + HEAD_SIZE].astype(BF16)
        key0 = rotate(early_ref[:, cols], cosine0, sine0).astype(BF16)
        value0 = early_ref[:, key_cols + j * HEAD_SIZE : key_cols + (j + 1) * HEAD_SIZE].astype(BF16)
        key_ref[:, cols], value_ref[:, cols] = key, value
        key0_ref[:, cols], value0_ref[:, cols] = key0, value0
        value_t, value0_t = flip(value), flip(value0)
        for h in range(j * group, (j + 1) * group):
            head_cols = slice(h * HEAD_SIZE, (h + 1) * HEAD_SIZE)
            query = rotate(proj_ref[:, head_cols], cosine, sine_part).astype(BF16)
            query_ref[:, head_cols] = query
            for first in range(0, rows, tile):
                last = first + tile
                q = query[first:last]
                s0 = dot_nt(key0, q) * factor + bias
                s1 = causal(dot_nt(key[:last], q) * factor, first)
                peak = jnp.maximum(
                    jnp.max(s0, axis=0, keepdims=True), jnp.max(s1, axis=0, keepdims=True)
                )
                w0, w1 = jnp.exp(s0 - peak), jnp.exp(s1 - peak)
                total = jnp.sum(w0, axis=0, keepdims=True) + jnp.sum(w1, axis=0, keepdims=True)
                scale = 1.0 / total
                mixed = dot_nn(value0_t, (w0 * scale).astype(BF16)) + dot_nn(
                    value_t[:, :last], (w1 * scale).astype(BF16)
                )
                attended_ref[first:last, head_cols] = mixed.T.astype(BF16)
                lse_ref[h : h + 1, first:last] = peak + jnp.log(total)
    attended = attended_ref[...]
    for at, weight in ((0, near_ref), (half, far_ref)):
        branch_ref[:, at : at + half] = dot_nt(attended, weight[:, out_cols]).astype(BF16)


def attend(place, low, high, piece, rest, near, far, tables, heads, group):
    rows, half = low.shape
    query_cols, key_cols = heads * group * HEAD_SIZE, heads * HEAD_SIZE
    return pl.pallas_call(
        functools.partial(attend_kernel, heads, group, rows // 2),
        out_shape=(
            shape(rows, half), shape(rows, half), shape(rows, query_cols), shape(rows, query_cols),
            shape(rows, key_cols), shape(rows, key_cols), shape(rows, key_cols), shape(rows, key_cols),
            shape(heads * group, rows, F32), shape(2, 2 * half, F32), shape(rows, 2 * half),
        ),
        in_specs=[SMEM] + [VMEM] * 10,
        out_specs=(VMEM,) * 11,
        scratch_shapes=[
            pltpu.VMEM((rows, query_cols + 2 * key_cols), F32), pltpu.VMEM((rows, 2 * key_cols), F32)
        ],
        cost_estimate=cost(2e10, 3e7),
        name="attend",
    )(place, low, high, piece, rest, near, far, *tables)


def attend_back_kernel(
    heads, group, tile, place_ref, query_ref, key_ref, value_ref, key0_ref, value0_ref, grad_ref, lse_ref,
    cos_ref, sin_ref, cos0_ref, sin0_ref, query_grad_ref, key_grad_ref, value_grad_ref, early_ref,
):
    factor = HEAD_SIZE ** (-0.5)
    rows = query_ref.shape[0]
    bias = jnp.where(place_ref[0] > 0, 0.0, NEG).astype(F32)
    cosine, sine_part, cosine0, sine0 = cos_ref[...], sin_ref[...], cos0_ref[...], sin0_ref[...]
    key_cols = heads * HEAD_SIZE
    tiles = rows // tile
    for j in range(heads):
        cols = slice(j * HEAD_SIZE, (j + 1) * HEAD_SIZE)
        key, value, key0, value0 = key_ref[:, cols], value_ref[:, cols], key0_ref[:, cols], value0_ref[:, cols]
        key_t, key0_t = flip(key), flip(key0)
        key_sum, value_sum = [0.0] * tiles, [0.0] * tiles
        key0_sum, value0_sum = 0.0, 0.0
        for h in range(j * group, (j + 1) * group):
            head_cols = slice(h * HEAD_SIZE, (h + 1) * HEAD_SIZE)
            query, grad = query_ref[:, head_cols], grad_ref[:, head_cols]
            for t in range(tiles):
                first, last = t * tile, (t + 1) * tile
                q, d = query[first:last], grad[first:last]
                lse = lse_ref[h : h + 1, first:last]
                p0 = jnp.exp(dot_nt(key0, q) * factor + (bias - lse))
                p1 = jnp.exp(causal(dot_nt(key[:last], q) * factor, first) - lse)
                g0, g1 = dot_nt(value0, d), dot_nt(value[:last], d)
                inner = jnp.sum(p0 * g0, axis=0, keepdims=True) + jnp.sum(p1 * g1, axis=0, keepdims=True)
                s0, s1 = (p0 * (g0 - inner)).astype(BF16), (p1 * (g1 - inner)).astype(BF16)
                query_part = (dot_nn(key0_t, s0) + dot_nn(key_t[:, :last], s1)).T * factor
                query_grad_ref[first:last, head_cols] = unrotate(
                    query_part, cosine[first:last], sine_part[first:last]
                ).astype(BF16)
                key0_sum += dot_nn(s0, q)
                value0_sum += dot_nn(p0.astype(BF16), d)
                key_part, value_part = dot_nn(s1, q), dot_nn(p1.astype(BF16), d)
                for u in range(t + 1):
                    key_sum[u] += key_part[u * tile : (u + 1) * tile]
                    value_sum[u] += value_part[u * tile : (u + 1) * tile]
        early_ref[:, cols] = unrotate(key0_sum * factor, cosine0, sine0).astype(BF16)
        early_ref[:, key_cols + j * HEAD_SIZE : key_cols + (j + 1) * HEAD_SIZE] = value0_sum.astype(BF16)
        for u in range(tiles):
            at = slice(u * tile, (u + 1) * tile)
            key_grad_ref[at, cols] = unrotate(key_sum[u] * factor, cosine[at], sine_part[at])
            value_grad_ref[at, cols] = value_sum[u]


def attend_back(place, query, key, value, key0, value0, grad, lse, tables, heads, group):
    rows, query_cols = query.shape
    key_cols = key.shape[1]
    return pl.pallas_call(
        functools.partial(attend_back_kernel, heads, group, rows // 2),
        out_shape=(
            shape(rows, query_cols), shape(rows, key_cols, F32), shape(rows, key_cols, F32),
            shape(rows, 2 * key_cols),
        ),
        in_specs=[SMEM] + [VMEM] * 11,
        out_specs=(VMEM,) * 4,
        cost_estimate=cost(2e10, 3e7),
        name="attend_back",
    )(place, query, key, value, key0, value0, grad, lse, *tables)


def forward_kernel(
    low_ref, high_ref, own_ref, other_ref, gain_ref, grad_low_ref, grad_high_ref,
    gate_near, gate_far, up_near, up_far, down_near, down_far,
    hidden_ref, gate_grad_ref, up_grad_ref, normed_low_ref, normed_high_ref, middle_ref,
    normed_grad_ref, result_ref, normed_sum, result_sum,
):
    step = pl.program_id(0)
    half = low_ref.shape[1]
    rows = low_ref.shape[0]

    @pl.when(step == 0)
    def _():
        gain = gain_ref[1:2, :]

        def body(at):
            x = jnp.concatenate([low_ref[at, :], high_ref[at, :]], axis=1).astype(F32)
            x = x + (own_ref[at, :].astype(F32) + other_ref[at, :].astype(F32))
            middle_ref[at, :] = x
            normed = (x * inverse_rms(x) * gain).astype(BF16)
            normed_low_ref[at, :] = normed[:, :half]
            normed_high_ref[at, :] = normed[:, half:]

        row_loop(rows, body)
        normed_sum[...] = jnp.zeros_like(normed_sum)
        result_sum[...] = jnp.zeros_like(result_sum)

    low, high = normed_low_ref[...], normed_high_ref[...]
    gate = dot_nn(low, gate_near[...]) + dot_nn(high, gate_far[...])
    up = dot_nn(low, up_near[...]) + dot_nn(high, up_far[...])
    hidden_grad = dot_nn(grad_low_ref[...], down_near[...]) + dot_nn(grad_high_ref[...], down_far[...])
    sigma = 1.0 / (1.0 + jnp.exp(-gate))
    swish = gate * sigma
    hidden = (swish * up).astype(BF16)
    gate_grad = (hidden_grad * up * sigma * (1.0 + gate * (1.0 - sigma))).astype(BF16)
    up_grad = (hidden_grad * swish).astype(BF16)
    hidden_ref[...] = hidden
    gate_grad_ref[...] = gate_grad
    up_grad_ref[...] = up_grad
    near, far = slice(0, half), slice(half, 2 * half)
    normed_sum[:, near] += dot_nt(gate_grad, gate_near[...]) + dot_nt(up_grad, up_near[...])
    normed_sum[:, far] += dot_nt(gate_grad, gate_far[...]) + dot_nt(up_grad, up_far[...])
    result_sum[:, near] += dot_nt(hidden, down_near[...])
    result_sum[:, far] += dot_nt(hidden, down_far[...])

    @pl.when(step == pl.num_programs(0) - 1)
    def _():
        normed_grad_ref[...] = normed_sum[...].astype(BF16)
        result_ref[...] = result_sum[...].astype(BF16)


def forward(low, high, own, other, gains, grad_low, grad_high, weights, tile=512):
    rows, half = low.shape
    units = weights[0].shape[1]
    tile = min(tile, units)
    whole = lambda cols, height=rows: pl.BlockSpec(
        (height, cols), lambda i: (0, 0), pipeline_mode=pl.Buffered(1)
    )
    kept = lambda cols: pl.BlockSpec((rows, cols), lambda i: (0, 0))
    weight = pl.BlockSpec((half, tile), lambda i: (0, i))
    cut = pl.BlockSpec((rows, tile), lambda i: (0, i))
    return pl.pallas_call(
        forward_kernel,
        grid=(units // tile,),
        out_shape=(
            shape(rows, units), shape(rows, units), shape(rows, units), shape(rows, half), shape(rows, half),
            shape(rows, 2 * half, F32), shape(rows, 2 * half), shape(rows, 2 * half),
        ),
        in_specs=[whole(half)] * 2 + [whole(2 * half)] * 2 + [whole(2 * half, 2)] + [whole(half)] * 2 + [weight] * 6,
        out_specs=(cut,) * 3 + (kept(half),) * 2 + (kept(2 * half),) * 3,
        scratch_shapes=[pltpu.VMEM((rows, 2 * half), F32)] * 2,
        cost_estimate=cost(12 * rows * units * 2 * half, 6e7),
        name="forward",
    )(low, high, own, other, gains, grad_low, grad_high, *weights)


def middle_kernel(
    own_ref, other_ref, middle_ref, gain_ref, grad_low_ref, grad_high_ref, near_ref, far_ref,
    middle_grad_ref, branch_low_ref, branch_high_ref, attended_grad_ref, gain_grad_ref,
):
    half = grad_low_ref.shape[1]
    gain = gain_ref[1:2, :]
    gain_grad_ref[...] = jnp.zeros_like(gain_grad_ref)

    def body(at):
        x = middle_ref[at, :]
        inverse = inverse_rms(x)
        plain = x * inverse
        own = own_ref[at, :].astype(F32)
        gain_grad_ref[...] += jnp.sum(own * plain, axis=0, keepdims=True)
        weighted = (own + other_ref[at, :].astype(F32)) * gain
        inner = jnp.mean(weighted * plain, axis=-1, keepdims=True)
        grad = jnp.concatenate([grad_low_ref[at, :], grad_high_ref[at, :]], axis=1).astype(F32)
        grad = grad + inverse * (weighted - plain * inner)
        middle_grad_ref[at, :] = grad
        branch_low_ref[at, :] = grad[:, :half].astype(BF16)
        branch_high_ref[at, :] = grad[:, half:].astype(BF16)

    row_loop(own_ref.shape[0], body)
    attended_grad_ref[...] = (
        dot_nn(branch_low_ref[...], near_ref[...]) + dot_nn(branch_high_ref[...], far_ref[...])
    ).astype(BF16)


def middle_back(own, other, middle, gains, grad_low, grad_high, near, far, query_cols, index):
    rows, half = grad_low.shape
    full = lambda a: pl.BlockSpec(a.shape, lambda i: (0, 0))
    out = lambda cols, height=rows: pl.BlockSpec((height, cols), lambda i: (0, 0))
    part = pl.BlockSpec((half, query_cols), lambda i: (0, index))
    return pl.pallas_call(
        middle_kernel,
        grid=(1,),
        out_shape=(
            shape(rows, 2 * half, F32), shape(rows, half), shape(rows, half), shape(rows, query_cols),
            shape(1, 2 * half, F32),
        ),
        in_specs=[full(a) for a in (own, other, middle, gains, grad_low, grad_high)] + [part, part],
        out_specs=(out(2 * half), out(half), out(half), out(query_cols), out(2 * half, 1)),
        cost_estimate=cost(4 * rows * half * query_cols, 2e7),
        name="middle_back",
    )(own, other, middle, gains, grad_low, grad_high, near, far)


def inputs_kernel(
    query_ref, key_ref, value_ref, later_ref, low_ref, high_ref, near_ref, far_ref,
    proj_grad_ref, send_ref, gain_grad_ref, own_ref,
):
    query_cols, key_cols = query_ref.shape[1], key_ref.shape[1]
    half = low_ref.shape[1]
    proj_grad_ref[:, :query_cols] = query_ref[...]
    for at, part in ((0, key_ref), (key_cols, value_ref)):
        proj_grad_ref[:, query_cols + at : query_cols + at + key_cols] = (
            part[...] + later_ref[:, at : at + key_cols].astype(F32)
        ).astype(BF16)
    grads = proj_grad_ref[...]
    own_ref[:, :half] = dot_nt(grads, near_ref[...])
    own_ref[:, half:] = dot_nt(grads, far_ref[...])
    gain_grad_ref[...] = jnp.zeros_like(gain_grad_ref)

    def body(at):
        x = jnp.concatenate([low_ref[at, :], high_ref[at, :]], axis=1).astype(F32)
        own = own_ref[at, :]
        gain_grad_ref[...] += jnp.sum(own * (x * inverse_rms(x)), axis=0, keepdims=True)
        send_ref[at, :] = own.astype(BF16)

    row_loop(query_ref.shape[0], body)


def inputs_back(query, key, value, later, low, high, near, far):
    rows, query_cols = query.shape
    half = low.shape[1]
    proj_cols = query_cols + 2 * key.shape[1]
    full = lambda a: pl.BlockSpec(a.shape, lambda i: (0, 0))
    out = lambda cols, height=rows: pl.BlockSpec((height, cols), lambda i: (0, 0))
    part = pl.BlockSpec((half, proj_cols), lambda i: (0, 0))
    return pl.pallas_call(
        inputs_kernel,
        grid=(1,),
        out_shape=(
            shape(rows, proj_cols), shape(rows, 2 * half), shape(1, 2 * half, F32)
        ),
        scratch_shapes=[pltpu.VMEM((rows, 2 * half), F32)],
        in_specs=[full(a) for a in (query, key, value, later, low, high)] + [part, part],
        out_specs=(out(proj_cols), out(2 * half), out(2 * half, 1)),
        cost_estimate=cost(4 * rows * half * proj_cols, 2e7),
        name="inputs_back",
    )(query, key, value, later, low, high, near, far)


def weight_grad_kernel(chips, left_ref, left_other_ref, right_ref, right_other_ref, own_ref, *rest):
    sends, (left_t, left_other_t) = rest[: chips - 1], rest[chips - 1 :]

    @pl.when(pl.program_id(0) == 0)
    def _():
        left_t[...] = flip(left_ref[...])
        left_other_t[...] = flip(left_other_ref[...])

    total = dot_nn(left_t[...], right_ref[...]) + dot_nn(left_other_t[...], right_other_ref[...])
    rows = own_ref.shape[0]
    own_ref[...] = total[:rows]
    for chip, send in enumerate(sends, 1):
        send[...] = total[chip * rows : (chip + 1) * rows].astype(BF16)


def weight_grad(left, left_other, right, right_other, rows, chips, name, tile=768):
    count, half = left.shape
    cols = right.shape[1]
    tile = tile if cols % tile == 0 else 512
    tile = min(tile, cols)
    fixed = pl.BlockSpec((count, half), lambda i: (0, 0), pipeline_mode=pl.Buffered(1))
    moving = pl.BlockSpec((count, tile), lambda i: (0, i))
    out = pl.BlockSpec((rows, tile), lambda i: (0, i))
    return pl.pallas_call(
        functools.partial(weight_grad_kernel, chips),
        grid=(cols // tile,),
        out_shape=(shape(rows, cols, F32),) + (shape(rows, cols),) * (chips - 1),
        in_specs=[fixed, fixed, moving, moving],
        out_specs=(out,) * chips,
        scratch_shapes=[pltpu.VMEM((half, count), BF16)] * 2,
        cost_estimate=cost(4 * count * half * cols, 2e7),
        name=name,
    )(left, left_other, right, right_other)


def over_context(array):
    return lax.ppermute(array, "context", [(0, 1), (1, 0)])


def over_tensor(array):
    return lax.ppermute(array, "tensor", [(0, 1), (1, 0)])


def context_half(total, axis=0):
    half = total.shape[axis] // 2
    own = lax.axis_index("context")
    keep = lax.dynamic_slice_in_dim(total, own * half, half, axis)
    send = lax.dynamic_slice_in_dim(total, (1 - own) * half, half, axis)
    return keep, send


def after(value, *earlier):
    return lax.optimization_barrier((value,) + earlier)[0]


class Plane:
    def __init__(self, width):
        self.count = lax.axis_size("shard")
        self.chips = self.count // 2
        self.rows = width // self.count
        self.half = width // 2

    def to_chip(self, array, chip):
        return lax.ppermute(array, "shard", [(i, i ^ (2 * chip)) for i in range(self.count)])

    def to_core(self, array):
        return lax.ppermute(array, "shard", [(i, i ^ 1) for i in range(self.count)])

    def fetch(self, array):
        return [array] + [self.to_chip(array, chip) for chip in range(1, self.chips)]

    def join(self, parts):
        near = jnp.concatenate(parts, axis=0)
        return near, self.to_core(near)

    def scatter(self, grads):
        total = grads[0]
        for chip in range(1, self.chips):
            total = total + self.to_chip(grads[chip], chip).astype(F32)
        keep, send = context_half(total)
        return keep + over_context(send.astype(BF16)).astype(F32)

    def gain_grads(self, stacked):
        stacked = stacked + over_tensor(stacked)
        stacked = stacked[:, : self.half] + self.to_core(stacked[:, self.half :])
        total = stacked[:, : self.rows]
        for chip in range(1, self.chips):
            total = total + self.to_chip(stacked[:, chip * self.rows : (chip + 1) * self.rows], chip)
        keep, send = context_half(total, 1)
        return keep + over_context(send)


def shards(
    tokens,
    attention_gain,
    query_weight,
    key_matrix,
    value_matrix,
    output_weight,
    feedforward_gain,
    gate_weight,
    up_weight,
    down_weight,
    cotangent,
):
    width = tokens.shape[-1]
    rows_local = tokens.shape[0] * tokens.shape[1]
    plane = Plane(width)
    rows, chips = plane.rows, plane.chips
    own_context, own_tensor = lax.axis_index("context"), lax.axis_index("tensor")
    me = lax.axis_index("shard")[None]
    place = jnp.stack([own_context, own_tensor])
    query_cols = query_weight.shape[1]
    key_cols = key_matrix.shape[1]
    heads = key_cols // HEAD_SIZE
    group = query_cols // key_cols
    tables = rotation(own_context * rows_local + jnp.arange(rows_local)) + rotation(jnp.arange(rows_local))

    gains = jnp.pad(jnp.stack([attention_gain, feedforward_gain], axis=1), ((0, 0), (0, LANES - 2)))
    pack = jnp.concatenate([query_weight, key_matrix, value_matrix, output_weight.T, gains], axis=1)
    pack_parts = plane.fetch(pack)
    low, high = enter(me, tokens.reshape(rows_local, width), rows, chips)
    piece = lax.ppermute(jnp.where(own_tensor == 0, low, high), "context", [(0, 1)])
    rest = over_tensor(piece)
    near, far = plane.join(pack_parts)
    gate_weight, up_weight = lax.optimization_barrier((gate_weight, up_weight, *pack_parts))[:2]
    gate_parts, up_parts = plane.fetch(gate_weight), plane.fetch(up_weight)
    down_parts = plane.fetch(after(down_weight.T, *gate_parts))
    grad_low, grad_high = enter(me, cotangent.reshape(rows_local, width), rows, chips)

    (
        normed_low, normed_high, attended, query, key, value, key0, value0, lse, gain_rows, branch
    ) = attend(place, low, high, piece, rest, near, far, tables, heads, group)
    branch_other = over_tensor(branch)
    weights = plane.join(gate_parts) + plane.join(up_parts) + plane.join(down_parts)
    (
        hidden, gate_grad, up_grad, normed2_low, normed2_high, middle, normed2_grad, result
    ) = forward(low, high, branch, branch_other, gain_rows, grad_low, grad_high, weights)
    normed2_other = over_tensor(normed2_grad)

    normed2_peer = plane.to_core(normed2_high)
    feed = [
        weight_grad(normed2_low, normed2_peer, gate_grad, plane.to_core(gate_grad), rows, chips, "gate_back"),
        weight_grad(normed2_low, normed2_peer, up_grad, plane.to_core(up_grad), rows, chips, "up_back"),
        weight_grad(grad_low, plane.to_core(grad_high), hidden, plane.to_core(hidden), rows, chips, "down_back"),
    ]
    normed2_other, *feed = lax.optimization_barrier((normed2_other, *feed))
    result_other = over_tensor(after(result, normed2_other))
    gate_weight_grad, up_weight_grad, down_weight_grad = (plane.scatter(grads) for grads in feed)

    middle_grad, branch_low, branch_high, attended_grad, gain_two = middle_back(
        normed2_grad, normed2_other, middle, gain_rows, grad_low, grad_high, near, far,
        query_cols, (query_cols + 2 * key_cols) // query_cols,
    )
    output_weight_grad = plane.scatter(
        weight_grad(branch_low, plane.to_core(branch_high), attended, plane.to_core(attended), rows, chips, "out_back")
    )
    query_grad, key_grad, value_grad, early = attend_back(
        place, query, key, value, key0, value0, attended_grad, lse, tables, heads, group
    )
    later = lax.ppermute(early, "context", [(1, 0)])
    proj_grad, normed1_grad, gain_one = inputs_back(
        query_grad, key_grad, value_grad, later, low, high, near, far
    )
    normed1_other = over_tensor(normed1_grad)
    proj_weight_grad = plane.scatter(
        weight_grad(
            normed_low, plane.to_core(normed_high), proj_grad, plane.to_core(proj_grad), rows, chips, "proj_back"
        )
    )
    gain_grads = plane.gain_grads(jnp.concatenate([gain_one, gain_two], axis=0))
    layer_output = leave(me, middle, result, result_other, rows, chips)
    input_grad = finish(me, normed1_grad, normed1_other, middle_grad, low, high, gain_rows, rows, chips)
    return (
        layer_output.reshape(tokens.shape),
        input_grad.reshape(tokens.shape),
        gain_grads[0],
        proj_weight_grad[:, :query_cols],
        proj_weight_grad[:, query_cols : query_cols + key_cols],
        proj_weight_grad[:, query_cols + key_cols :],
        output_weight_grad.T,
        gain_grads[1],
        gate_weight_grad,
        up_weight_grad,
        down_weight_grad.T,
    )


def solution(mesh):
    in_specs = (
        P("shard", "context", None),
        P("shard"),
        P("shard", "tensor"),
        P("shard", "tensor"),
        P("shard", "tensor"),
        P("tensor", "shard"),
        P("shard"),
        P("shard", "tensor"),
        P("shard", "tensor"),
        P("tensor", "shard"),
        P("shard", "context", None),
    )
    out_specs = (
        P("shard", "context", None),
        P("shard", "context", None),
        P(("shard", "context")),
        P(("shard", "context"), "tensor"),
        P(("shard", "context"), "tensor"),
        P(("shard", "context"), "tensor"),
        P("tensor", ("shard", "context")),
        P(("shard", "context")),
        P(("shard", "context"), "tensor"),
        P(("shard", "context"), "tensor"),
        P("tensor", ("shard", "context")),
    )
    return jax.shard_map(shards, mesh=mesh, in_specs=in_specs, out_specs=out_specs, check_vma=False)
```

```python
import functools

import jax
import jax.numpy as jnp
from jax import lax
from jax.experimental import pallas as pl
from jax.experimental.pallas import tpu as pltpu
from jax.sharding import PartitionSpec as P


HEAD_SIZE = 96
EPS = 1e-05
THETA = 100000.0
BF16 = jnp.bfloat16
F32 = jnp.float32
NEG = -1e30
LANES = 128


VMEM = pl.BlockSpec(memory_space=pltpu.VMEM)
SMEM = pl.BlockSpec(memory_space=pltpu.SMEM)


def shape(rows, cols, kind=BF16):
    return jax.ShapeDtypeStruct((rows, cols), kind)


def cost(flops, moved):
    return pl.CostEstimate(flops=int(flops), bytes_accessed=int(moved), transcendentals=0)


def rotation(positions):
    half_dim = HEAD_SIZE // 2
    spin_rates = THETA ** (-jnp.arange(half_dim, dtype=F32) * 2.0 / HEAD_SIZE)
    angles = positions.astype(F32)[:, None] * spin_rates[None, :]
    angles = jnp.concatenate([angles, angles], axis=-1)
    return (jnp.cos(angles), jnp.sin(angles))


def dot_nn(a, b):
    return lax.dot_general(a, b, (((1,), (0,)), ((), ())), preferred_element_type=F32)


def dot_nt(a, b):
    return lax.dot_general(a, b, (((1,), (1,)), ((), ())), preferred_element_type=F32)


def flip(a):
    return a.astype(F32).T.astype(a.dtype)


def rotate(v, cosine, sine_part):
    half_dim = HEAD_SIZE // 2
    turned = jnp.concatenate([-v[:, half_dim:], v[:, :half_dim]], axis=1)
    return v * cosine + turned * sine_part


def unrotate(u, cosine, sine_part):
    half_dim = HEAD_SIZE // 2
    s = u * sine_part
    return u * cosine + jnp.concatenate([s[:, half_dim:], -s[:, :half_dim]], axis=1)


def causal(scores, first):
    keys = lax.broadcasted_iota(jnp.int32, scores.shape, 0)
    queries = lax.broadcasted_iota(jnp.int32, scores.shape, 1)
    return jnp.where(keys <= queries + first, scores, NEG)


def inverse_rms(x):
    return lax.rsqrt(jnp.mean(x * x, axis=-1, keepdims=True) + EPS)


def exchange_blocks(x, me, rows):
    width = x.shape[1]
    step, bit = width // 2, me % 2
    while True:
        parts = []
        for first in range(0, width, 2 * step):
            parts += [x[:, first + step : first + 2 * step], x[:, first : first + step]]
        x = jnp.where(bit > 0, jnp.concatenate(parts, axis=1), x)
        step //= 2
        if step < rows:
            return x
        bit = (me // 2) // (step // rows) % 2


def to_relative(x, me, rows, chips):
    blocks = [
        x[:, (chip * 2 + core) * rows : (chip * 2 + core + 1) * rows]
        for core in range(2)
        for chip in range(chips)
    ]
    return exchange_blocks(jnp.concatenate(blocks, axis=1), me, rows)


def to_absolute(x, me, rows, chips):
    x = exchange_blocks(x, me, rows)
    blocks = [
        x[:, (core * chips + chip) * rows : (core * chips + chip + 1) * rows]
        for chip in range(chips)
        for core in range(2)
    ]
    return jnp.concatenate(blocks, axis=1)


def row_loop(total, body, step=64):
    def one(i, carry):
        body(pl.ds(pl.multiple_of(i * step, step), step))
        return carry

    lax.fori_loop(0, total // step, one, 0)


def row_block(rows, cols, first=0):
    return pl.BlockSpec((rows, cols), lambda i: (first + i, 0))


def fixed_block(rows, cols):
    return pl.BlockSpec((rows, cols), lambda i: (0, 0))


def enter_kernel(rows, chips, me_ref, tokens_ref, low_ref, high_ref):
    half = low_ref.shape[1]

    def body(at):
        x = to_relative(tokens_ref[at, :].astype(F32), me_ref[0], rows, chips).astype(BF16)
        low_ref[at, :] = x[:, :half]
        high_ref[at, :] = x[:, half:]

    row_loop(tokens_ref.shape[0], body)


def enter(me, tokens, rows, chips, block=128):
    count, width = tokens.shape
    return pl.pallas_call(
        functools.partial(enter_kernel, rows, chips),
        grid=(count // block,),
        out_shape=(shape(count, width // 2),) * 2,
        in_specs=[SMEM, row_block(block, width)],
        out_specs=(row_block(block, width // 2),) * 2,
        cost_estimate=cost(0, 6 * count * width),
    )(me, tokens)


def leave_kernel(rows, chips, me_ref, middle_ref, own_ref, other_ref, out_ref):
    def body(at):
        x = middle_ref[at, :] + (own_ref[at, :].astype(F32) + other_ref[at, :].astype(F32))
        out_ref[at, :] = to_absolute(x, me_ref[0], rows, chips).astype(BF16)

    row_loop(own_ref.shape[0], body)


def leave(me, middle, own, other, rows, chips, block=128):
    count, width = own.shape
    return pl.pallas_call(
        functools.partial(leave_kernel, rows, chips),
        grid=(count // block,),
        out_shape=shape(*own.shape),
        in_specs=[SMEM] + [row_block(block, width)] * 3,
        out_specs=row_block(block, width),
        cost_estimate=cost(0, 8 * own.size),
        name="kl",
    )(me, middle, own, other)


def finish_kernel(rows, chips, me_ref, own_ref, other_ref, grad_ref, low_ref, high_ref, gain_ref, *rest):
    out_ref = rest[-1]
    gain = gain_ref[0:1, :]

    def body(at):
        x = jnp.concatenate([low_ref[at, :], high_ref[at, :]], axis=1).astype(F32)
        inverse = inverse_rms(x)
        plain = x * inverse
        weighted = (own_ref[at, :].astype(F32) + other_ref[at, :].astype(F32)) * gain
        inner = jnp.mean(weighted * plain, axis=-1, keepdims=True)
        grad = grad_ref[at, :] + inverse * (weighted - plain * inner)
        out_ref[at, :] = to_absolute(grad, me_ref[0], rows, chips)

    row_loop(own_ref.shape[0], body)


def finish(me, own, other, grad, low, high, gains, rows, chips, part, before, block=64):
    count, width = own.shape
    first = part * (count // block)
    later = () if before is None else (before,)
    return pl.pallas_call(
        functools.partial(finish_kernel, rows, chips),
        grid=(count // block,),
        out_shape=shape(*grad.shape, F32),
        in_specs=[SMEM, row_block(block, width), row_block(block, width), row_block(block, width, first)]
        + [row_block(block, width // 2, first)] * 2
        + [fixed_block(2, width)]
        + [pl.BlockSpec(memory_space=pl.ANY)] * len(later),
        out_specs=row_block(block, width, first),
        input_output_aliases={7: 0} if later else {},
        cost_estimate=cost(0, 16 * own.size),
    )(me, own, other, grad, low, high, gains, *later)


def normed_halves(low, high, gain):
    half = low.shape[1]
    x = jnp.concatenate([low, high], axis=1).astype(F32)
    x = (x * inverse_rms(x) * gain).astype(BF16)
    return x[:, :half], x[:, half:]


def project_kernel(
    proj_cols, gain_at, low_ref, high_ref, near_ref, far_ref, normed_low_ref, normed_high_ref, gain_ref, proj_ref
):
    gain_cols = slice(gain_at, gain_at + LANES)
    gain_ref[...] = jnp.concatenate(
        [near_ref[:, gain_cols].astype(F32).T[0:2], far_ref[:, gain_cols].astype(F32).T[0:2]], axis=1
    )
    low, high = normed_halves(low_ref[...], high_ref[...], gain_ref[0:1, :])
    normed_low_ref[...] = low
    normed_high_ref[...] = high
    proj_ref[...] = dot_nn(low, near_ref[:, :proj_cols]) + dot_nn(high, far_ref[:, :proj_cols])


def project(low, high, near, far, proj_cols):
    rows, half = low.shape
    return pl.pallas_call(
        functools.partial(project_kernel, proj_cols, near.shape[1] - LANES),
        out_shape=(shape(rows, half), shape(rows, half), shape(2, 2 * half, F32), shape(rows, proj_cols, F32)),
        in_specs=[VMEM] * 4,
        out_specs=(VMEM,) * 4,
        cost_estimate=cost(4 * rows * half * proj_cols, 2e7),
        name="kp",
    )(low, high, near, far)


def attend_kernel(
    heads, group, tile, place_ref, proj_ref, gain_ref, *rest_refs
):
    pieces = (len(rest_refs) - 17) // 2
    piece_refs, other_refs = rest_refs[:pieces], rest_refs[pieces : 2 * pieces]
    (
        near_ref, far_ref, cos_ref, sin_ref, cos0_ref, sin0_ref,
        attended_ref, query_ref, key_ref, value_ref, key0_ref, value0_ref, lse_ref, branch_ref,
        normed0_low_ref, normed0_high_ref, early_ref,
    ) = rest_refs[2 * pieces :]
    factor = HEAD_SIZE ** (-0.5)
    rows = proj_ref.shape[0]
    half = near_ref.shape[0]
    query_cols = heads * group * HEAD_SIZE
    key_cols = heads * HEAD_SIZE
    proj_cols = query_cols + 2 * key_cols
    out_cols = slice(proj_cols, proj_cols + query_cols)
    first_piece = place_ref[1] == 0
    at = 0
    for piece_ref, other_ref in zip(piece_refs, other_refs):
        piece, other = piece_ref[...].astype(F32), other_ref[...].astype(F32)
        low, high = normed_halves(
            jnp.where(first_piece, piece, other), jnp.where(first_piece, other, piece), gain_ref[0:1, :]
        )
        normed0_low_ref[at : at + piece.shape[0], :] = low
        normed0_high_ref[at : at + piece.shape[0], :] = high
        early_ref[at : at + piece.shape[0], :] = dot_nn(low, near_ref[:, query_cols:proj_cols]) + dot_nn(
            high, far_ref[:, query_cols:proj_cols]
        )
        at += piece.shape[0]
    bias = jnp.where(place_ref[0] > 0, 0.0, NEG).astype(F32)
    cosine, sine_part, cosine0, sine0 = cos_ref[...], sin_ref[...], cos0_ref[...], sin0_ref[...]
    for j in range(heads):
        cols = slice(j * HEAD_SIZE, (j + 1) * HEAD_SIZE)
        start = query_cols + j * HEAD_SIZE
        key = rotate(proj_ref[:, start : start + HEAD_SIZE], cosine, sine_part).astype(BF16)
        start += key_cols
        value = proj_ref[:, start : start + HEAD_SIZE].astype(BF16)
        key0 = rotate(early_ref[:, cols], cosine0, sine0).astype(BF16)
        value0 = early_ref[:, key_cols + j * HEAD_SIZE : key_cols + (j + 1) * HEAD_SIZE].astype(BF16)
        key_ref[:, cols], value_ref[:, cols] = key, value
        key0_ref[:, cols], value0_ref[:, cols] = key0, value0
        value_t, value0_t = flip(value), flip(value0)
        for h in range(j * group, (j + 1) * group):
            head_cols = slice(h * HEAD_SIZE, (h + 1) * HEAD_SIZE)
            query = rotate(proj_ref[:, head_cols], cosine, sine_part).astype(BF16)
            query_ref[:, head_cols] = query
            for first in range(0, rows, tile):
                last = first + tile
                q = query[first:last]
                s0 = dot_nt(key0, q) * factor + bias
                s1 = causal(dot_nt(key[:last], q) * factor, first)
                peak = jnp.maximum(
                    jnp.max(s0, axis=0, keepdims=True), jnp.max(s1, axis=0, keepdims=True)
                )
                w0, w1 = jnp.exp(s0 - peak), jnp.exp(s1 - peak)
                total = jnp.sum(w0, axis=0, keepdims=True) + jnp.sum(w1, axis=0, keepdims=True)
                scale = 1.0 / total
                mixed = dot_nn(value0_t, (w0 * scale).astype(BF16)) + dot_nn(
                    value_t[:, :last], (w1 * scale).astype(BF16)
                )
                attended_ref[first:last, head_cols] = mixed.T.astype(BF16)
                lse_ref[h : h + 1, first:last] = peak + jnp.log(total)
    attended = attended_ref[...]
    for at, weight in ((0, near_ref), (half, far_ref)):
        branch_ref[:, at : at + half] = dot_nt(attended, weight[:, out_cols]).astype(BF16)


def attend(place, proj, gains, pieces, others, near, far, tables, heads, group):
    rows = proj.shape[0]
    half = near.shape[0]
    query_cols, key_cols = heads * group * HEAD_SIZE, heads * HEAD_SIZE
    return pl.pallas_call(
        functools.partial(attend_kernel, heads, group, rows // 2),
        out_shape=(
            shape(rows, query_cols), shape(rows, query_cols),
            shape(rows, key_cols), shape(rows, key_cols), shape(rows, key_cols), shape(rows, key_cols),
            shape(heads * group, rows, F32), shape(rows, 2 * half), shape(rows, half), shape(rows, half),
        ),
        in_specs=[SMEM] + [VMEM] * (8 + 2 * len(pieces)),
        out_specs=(VMEM,) * 10,
        scratch_shapes=[pltpu.VMEM((rows, 2 * key_cols), F32)],
        cost_estimate=cost(2e10, 3e7),
        name="ka",
    )(place, proj, gains, *pieces, *others, near, far, *tables)


def attend_back_kernel(
    head_range, group, tile, place_ref, query_ref, key_ref, value_ref, key0_ref, value0_ref, grad_ref, lse_ref,
    cos_ref, sin_ref, cos0_ref, sin0_ref, early_ref, grads_ref,
):
    factor = HEAD_SIZE ** (-0.5)
    rows = query_ref.shape[0]
    bias = jnp.where(place_ref[0] > 0, 0.0, NEG).astype(F32)
    cosine, sine_part, cosine0, sine0 = cos_ref[...], sin_ref[...], cos0_ref[...], sin0_ref[...]
    start = head_range[0]
    key_cols = len(head_range) * HEAD_SIZE
    query_cols = key_cols * group
    tiles = rows // tile
    for j in head_range:
        cols = slice(j * HEAD_SIZE, (j + 1) * HEAD_SIZE)
        key, value, key0, value0 = key_ref[:, cols], value_ref[:, cols], key0_ref[:, cols], value0_ref[:, cols]
        key_t, key0_t = flip(key), flip(key0)
        key_sum, value_sum = [0.0] * tiles, [0.0] * tiles
        key0_sum, value0_sum = 0.0, 0.0
        for h in range(j * group, (j + 1) * group):
            head_cols = slice(h * HEAD_SIZE, (h + 1) * HEAD_SIZE)
            query, grad = query_ref[:, head_cols], grad_ref[:, head_cols]
            for t in range(tiles):
                first, last = t * tile, (t + 1) * tile
                q, d = query[first:last], grad[first:last]
                lse = lse_ref[h : h + 1, first:last]
                p0 = jnp.exp(dot_nt(key0, q) * factor + (bias - lse))
                p1 = jnp.exp(causal(dot_nt(key[:last], q) * factor, first) - lse)
                g0, g1 = dot_nt(value0, d), dot_nt(value[:last], d)
                inner = jnp.sum(p0 * g0, axis=0, keepdims=True) + jnp.sum(p1 * g1, axis=0, keepdims=True)
                s0, s1 = (p0 * (g0 - inner)).astype(BF16), (p1 * (g1 - inner)).astype(BF16)
                query_part = (dot_nn(key0_t, s0) + dot_nn(key_t[:, :last], s1)).T * factor
                at_cols = slice((h - start * group) * HEAD_SIZE, (h - start * group + 1) * HEAD_SIZE)
                grads_ref[first:last, at_cols] = unrotate(
                    query_part, cosine[first:last], sine_part[first:last]
                ).astype(BF16)
                key0_sum += dot_nn(s0, q)
                value0_sum += dot_nn(p0.astype(BF16), d)
                key_part, value_part = dot_nn(s1, q), dot_nn(p1.astype(BF16), d)
                for u in range(t + 1):
                    key_sum[u] += key_part[u * tile : (u + 1) * tile]
                    value_sum[u] += value_part[u * tile : (u + 1) * tile]
        near = (j - start) * HEAD_SIZE
        key_at = query_cols + near
        value_at = key_at + key_cols
        for u in range(tiles):
            at = slice(u * tile, (u + 1) * tile)
            grads_ref[at, key_at : key_at + HEAD_SIZE] = unrotate(
                key_sum[u] * factor, cosine[at], sine_part[at]
            ).astype(BF16)
            grads_ref[at, value_at : value_at + HEAD_SIZE] = value_sum[u].astype(BF16)
        early_ref[:, near : near + HEAD_SIZE] = unrotate(key0_sum * factor, cosine0, sine0).astype(BF16)
        early_ref[:, key_cols + near : key_cols + near + HEAD_SIZE] = value0_sum.astype(BF16)
    grads_ref[:, query_cols + 2 * key_cols :] = early_ref[...]


def attend_back(place, query, key, value, key0, value0, grad, lse, tables, head_range, group):
    rows = query.shape[0]
    key_cols = len(head_range) * HEAD_SIZE
    return pl.pallas_call(
        functools.partial(attend_back_kernel, head_range, group, rows // 2),
        out_shape=(shape(rows, 2 * key_cols), shape(rows, (group + 4) * key_cols)),
        in_specs=[SMEM] + [VMEM] * 11,
        out_specs=(VMEM,) * 2,
        cost_estimate=cost(1e10, 3e7),
    )(place, query, key, value, key0, value0, grad, lse, *tables)


def join_grads(parts, group):
    unit = parts[0].shape[1] // (group + 4)
    parts = [part.astype(F32) for part in parts]

    def take(first, last):
        return [part[:, first * unit : last * unit] for part in parts]

    query = take(0, group)
    rest = take(group, group + 1) + take(group + 1, group + 2)
    early = take(group + 2, group + 3) + take(group + 3, group + 4)
    return [jnp.concatenate(list_, axis=1).astype(BF16) for list_ in (query, rest, early)]


def forward_kernel(
    low_ref, high_ref, own_ref, other_ref, gain_ref, grad_low_ref, grad_high_ref,
    gate_near, gate_far, up_near, up_far, down_near, down_far,
    hidden_ref, gate_grad_ref, up_grad_ref, normed_low_ref, normed_high_ref, middle_ref,
    normed_grad_ref, result_ref, normed_sum, result_sum,
):
    step = pl.program_id(0)
    half = low_ref.shape[1]
    rows = low_ref.shape[0]

    @pl.when(step == 0)
    def _():
        gain = gain_ref[1:2, :]

        def body(at):
            x = jnp.concatenate([low_ref[at, :], high_ref[at, :]], axis=1).astype(F32)
            x = x + (own_ref[at, :].astype(F32) + other_ref[at, :].astype(F32))
            middle_ref[at, :] = x
            normed = (x * inverse_rms(x) * gain).astype(BF16)
            normed_low_ref[at, :] = normed[:, :half]
            normed_high_ref[at, :] = normed[:, half:]

        row_loop(rows, body)
        normed_sum[...] = jnp.zeros_like(normed_sum)
        result_sum[...] = jnp.zeros_like(result_sum)

    low, high = normed_low_ref[...], normed_high_ref[...]
    gate = dot_nn(low, gate_near[...]) + dot_nn(high, gate_far[...])
    up = dot_nn(low, up_near[...]) + dot_nn(high, up_far[...])
    hidden_grad = dot_nn(grad_low_ref[...], down_near[...]) + dot_nn(grad_high_ref[...], down_far[...])
    sigma = 1.0 / (1.0 + jnp.exp(-gate))
    swish = gate * sigma
    hidden = (swish * up).astype(BF16)
    gate_grad = (hidden_grad * up * sigma * (1.0 + gate * (1.0 - sigma))).astype(BF16)
    up_grad = (hidden_grad * swish).astype(BF16)
    hidden_ref[...] = hidden
    gate_grad_ref[...] = gate_grad
    up_grad_ref[...] = up_grad
    near, far = slice(0, half), slice(half, 2 * half)
    normed_sum[:, near] += dot_nt(gate_grad, gate_near[...]) + dot_nt(up_grad, up_near[...])
    normed_sum[:, far] += dot_nt(gate_grad, gate_far[...]) + dot_nt(up_grad, up_far[...])
    result_sum[:, near] += dot_nt(hidden, down_near[...])
    result_sum[:, far] += dot_nt(hidden, down_far[...])

    @pl.when(step == pl.num_programs(0) - 1)
    def _():
        normed_grad_ref[...] = normed_sum[...].astype(BF16)
        result_ref[...] = result_sum[...].astype(BF16)


def forward(low, high, own, other, gains, grad_low, grad_high, weights, tile=512):
    rows, half = low.shape
    units = weights[0].shape[1]
    tile = min(tile, units)
    whole = lambda cols, height=rows: pl.BlockSpec(
        (height, cols), lambda i: (0, 0), pipeline_mode=pl.Buffered(1)
    )
    kept = lambda cols: pl.BlockSpec((rows, cols), lambda i: (0, 0))
    weight = pl.BlockSpec((half, tile), lambda i: (0, i))
    cut = pl.BlockSpec((rows, tile), lambda i: (0, i))
    return pl.pallas_call(
        forward_kernel,
        grid=(units // tile,),
        out_shape=(
            shape(rows, units), shape(rows, units), shape(rows, units), shape(rows, half), shape(rows, half),
            shape(rows, 2 * half, F32), shape(rows, 2 * half), shape(rows, 2 * half),
        ),
        in_specs=[whole(half)] * 2 + [whole(2 * half)] * 2 + [whole(2 * half, 2)] + [whole(half)] * 2 + [weight] * 6,
        out_specs=(cut,) * 3 + (kept(half),) * 2 + (kept(2 * half),) * 3,
        scratch_shapes=[pltpu.VMEM((rows, 2 * half), F32)] * 2,
        cost_estimate=cost(12 * rows * units * 2 * half, 6e7),
        name="kf",
    )(low, high, own, other, gains, grad_low, grad_high, *weights)


def middle_kernel(
    own_ref, other_ref, middle_ref, gain_ref, grad_low_ref, grad_high_ref, near_ref, far_ref,
    middle_grad_ref, branch_low_ref, branch_high_ref, attended_grad_ref, gain_grad_ref,
):
    half = grad_low_ref.shape[1]
    gain = gain_ref[1:2, :]

    @pl.when(pl.program_id(0) == 0)
    def _():
        gain_grad_ref[...] = jnp.zeros_like(gain_grad_ref)

    def body(at):
        x = middle_ref[at, :]
        inverse = inverse_rms(x)
        plain = x * inverse
        own = own_ref[at, :].astype(F32)
        gain_grad_ref[...] += jnp.sum(own * plain, axis=0, keepdims=True)
        weighted = (own + other_ref[at, :].astype(F32)) * gain
        inner = jnp.mean(weighted * plain, axis=-1, keepdims=True)
        grad = jnp.concatenate([grad_low_ref[at, :], grad_high_ref[at, :]], axis=1).astype(F32)
        grad = grad + inverse * (weighted - plain * inner)
        middle_grad_ref[at, :] = grad
        branch_low_ref[at, :] = grad[:, :half].astype(BF16)
        branch_high_ref[at, :] = grad[:, half:].astype(BF16)

    row_loop(own_ref.shape[0], body)
    attended_grad_ref[...] = (
        dot_nn(branch_low_ref[...], near_ref[...]) + dot_nn(branch_high_ref[...], far_ref[...])
    ).astype(BF16)


def middle_back(own, other, middle, gains, grad_low, grad_high, near, far, query_cols, index, block=128):
    rows, half = grad_low.shape
    part = pl.BlockSpec((half, query_cols), lambda i: (0, index))
    wide, narrow = row_block(block, 2 * half), row_block(block, half)
    return pl.pallas_call(
        middle_kernel,
        grid=(rows // block,),
        out_shape=(
            shape(rows, 2 * half, F32), shape(rows, half), shape(rows, half), shape(rows, query_cols),
            shape(1, 2 * half, F32),
        ),
        in_specs=[wide, wide, wide, fixed_block(2, 2 * half), narrow, narrow, part, part],
        out_specs=(wide, narrow, narrow, row_block(block, query_cols), fixed_block(1, 2 * half)),
        cost_estimate=cost(4 * rows * half * query_cols, 2e7),
        name="km",
    )(own, other, middle, gains, grad_low, grad_high, near, far)


def inputs_kernel(group, count, *refs):
    grad_refs, later_refs = refs[:count], refs[count : 2 * count]
    low_ref, high_ref, near_ref, far_ref, send_ref, gain_grad_ref, own_ref = refs[2 * count :]
    half = low_ref.shape[1]
    query, rest, _ = join_grads([ref[...] for ref in grad_refs], group)
    query_cols = query.shape[1]
    later = [ref[...].astype(F32) for ref in later_refs]
    unit = later[0].shape[1] // 2
    later = jnp.concatenate([a[:, :unit] for a in later] + [a[:, unit:] for a in later], axis=1)
    rest = (rest.astype(F32) + later).astype(BF16)
    for at, weight in ((0, near_ref), (half, far_ref)):
        own_ref[:, at : at + half] = dot_nt(query, weight[:, :query_cols]) + dot_nt(rest, weight[:, query_cols:])
    gain_grad_ref[...] = jnp.zeros_like(gain_grad_ref)

    def body(at):
        x = jnp.concatenate([low_ref[at, :], high_ref[at, :]], axis=1).astype(F32)
        own = own_ref[at, :]
        gain_grad_ref[...] += jnp.sum(own * (x * inverse_rms(x)), axis=0, keepdims=True)
        send_ref[at, :] = own.astype(BF16)

    row_loop(low_ref.shape[0], body)


def inputs_back(grads, later, low, high, near, far, group, proj_cols, part, parts):
    rows, half = low.shape
    block = rows // parts
    weight = fixed_block(half, proj_cols)
    return pl.pallas_call(
        functools.partial(inputs_kernel, group, len(grads)),
        grid=(1,),
        out_shape=(shape(block, 2 * half), shape(1, 2 * half, F32)),
        scratch_shapes=[pltpu.VMEM((block, 2 * half), F32)],
        in_specs=[row_block(block, a.shape[1], part) for a in (*grads, *later, low, high)] + [weight, weight],
        out_specs=(fixed_block(block, 2 * half), fixed_block(1, 2 * half)),
        cost_estimate=cost(4 * block * half * proj_cols, 2e7),
    )(*grads, *later, low, high, near, far)


def proj_grad_kernel(group, count, left_ref, left_peer_ref, left0_ref, left0_peer_ref, *refs):
    grads = join_grads([ref[...] for ref in refs[:count]], group)
    peers = join_grads([ref[...] for ref in refs[count : 2 * count]], group)
    own_ref, *sends = refs[2 * count :]
    rows = own_ref.shape[0]
    left, left_peer = flip(left_ref[...]), flip(left_peer_ref[...])
    left0, left0_peer = flip(left0_ref[...]), flip(left0_peer_ref[...])
    at = 0
    for index in range(2):
        total = dot_nn(left, grads[index]) + dot_nn(left_peer, peers[index])
        if index:
            total = total + dot_nn(left0, grads[2]) + dot_nn(left0_peer, peers[2])
        cols = slice(at, at + total.shape[1])
        own_ref[:, cols] = total[:rows]
        for chip, send in enumerate(sends, 1):
            send[:, cols] = total[chip * rows : (chip + 1) * rows].astype(BF16)
        at = cols.stop


def proj_grad(left, left_peer, left0, left0_peer, grads, peers, rows, chips, group, proj_cols):
    return pl.pallas_call(
        functools.partial(proj_grad_kernel, group, len(grads)),
        out_shape=(shape(rows, proj_cols, F32),) + (shape(rows, proj_cols),) * (chips - 1),
        in_specs=[VMEM] * (4 + 2 * len(grads)),
        out_specs=(VMEM,) * chips,
        cost_estimate=cost(6e9, 2e7),
        name="kj",
    )(left, left_peer, left0, left0_peer, *grads, *peers)


def weight_grad_kernel(chips, left_ref, left_other_ref, right_ref, right_other_ref, own_ref, *rest):
    sends, (left_t, left_other_t) = rest[: chips - 1], rest[chips - 1 :]

    @pl.when(pl.program_id(0) == 0)
    def _():
        left_t[...] = flip(left_ref[...])
        left_other_t[...] = flip(left_other_ref[...])

    total = dot_nn(left_t[...], right_ref[...]) + dot_nn(left_other_t[...], right_other_ref[...])
    rows = own_ref.shape[0]
    own_ref[...] = total[:rows]
    for chip, send in enumerate(sends, 1):
        send[...] = total[chip * rows : (chip + 1) * rows].astype(BF16)


def weight_grad(left, left_other, right, right_other, rows, chips, tile=768):
    count, half = left.shape
    cols = right.shape[1]
    tile = tile if cols % tile == 0 else 512
    tile = min(tile, cols)
    fixed = pl.BlockSpec((count, half), lambda i: (0, 0), pipeline_mode=pl.Buffered(1))
    moving = pl.BlockSpec((count, tile), lambda i: (0, i))
    out = pl.BlockSpec((rows, tile), lambda i: (0, i))
    return pl.pallas_call(
        functools.partial(weight_grad_kernel, chips),
        grid=(cols // tile,),
        out_shape=(shape(rows, cols, F32),) + (shape(rows, cols),) * (chips - 1),
        in_specs=[fixed, fixed, moving, moving],
        out_specs=(out,) * chips,
        scratch_shapes=[pltpu.VMEM((half, count), BF16)] * 2,
        cost_estimate=cost(4 * count * half * cols, 2e7),
    )(left, left_other, right, right_other)


def over_context(array):
    return lax.ppermute(array, "context", [(0, 1), (1, 0)])


def over_tensor(array):
    return lax.ppermute(array, "tensor", [(0, 1), (1, 0)])


def context_half(total, axis=0):
    half = total.shape[axis] // 2
    own = lax.axis_index("context")
    keep = lax.dynamic_slice_in_dim(total, own * half, half, axis)
    send = lax.dynamic_slice_in_dim(total, (1 - own) * half, half, axis)
    return keep, send


class Plane:
    def __init__(self, width):
        self.count = lax.axis_size("shard")
        self.chips = self.count // 2
        self.rows = width // self.count
        self.half = width // 2

    def to_chip(self, array, chip):
        return lax.ppermute(array, "shard", [(i, i ^ (2 * chip)) for i in range(self.count)])

    def to_core(self, array):
        return lax.ppermute(array, "shard", [(i, i ^ 1) for i in range(self.count)])

    def fetch(self, array):
        if self.chips != 4:
            return [array] + [self.to_chip(array, chip) for chip in range(1, self.chips)]
        cut = self.rows // 2
        first, second = self.to_chip(array, 1), self.to_chip(array, 2)
        return [array, first, second, self.to_chip(first[:cut], 2), self.to_chip(second[cut:], 1)]

    def join(self, parts):
        near = jnp.concatenate(parts, axis=0)
        return near, self.to_core(near)

    def scatter(self, grads):
        total = grads[0]
        for chip in range(1, self.chips):
            total = total + self.to_chip(grads[chip], chip).astype(F32)
        keep, send = context_half(total)
        return keep + over_context(send.astype(BF16)).astype(F32)

    def gain_grads(self, stacked):
        stacked = stacked[:, : self.half] + self.to_core(stacked[:, self.half :])
        total = stacked[:, : self.rows]
        for chip in range(1, self.chips):
            piece = stacked[:, chip * self.rows : (chip + 1) * self.rows]
            total = total + self.to_chip(piece, chip)
        keep, send = context_half(total, 1)
        other = lax.ppermute(send, ("context", "tensor"), [(i, i ^ 3) for i in range(4)])
        return (keep + over_tensor(keep)) + (over_context(send) + other)


def shards(
    tokens,
    attention_gain,
    query_weight,
    key_matrix,
    value_matrix,
    output_weight,
    feedforward_gain,
    gate_weight,
    up_weight,
    down_weight,
    cotangent,
):
    width = tokens.shape[-1]
    rows_local = tokens.shape[0] * tokens.shape[1]
    plane = Plane(width)
    rows, chips = plane.rows, plane.chips
    own_context, own_tensor = lax.axis_index("context"), lax.axis_index("tensor")
    me = lax.axis_index("shard")[None]
    place = jnp.stack([own_context, own_tensor])
    query_cols = query_weight.shape[1]
    key_cols = key_matrix.shape[1]
    heads = key_cols // HEAD_SIZE
    group = query_cols // key_cols
    tables = rotation(own_context * rows_local + jnp.arange(rows_local)) + rotation(jnp.arange(rows_local))

    gains = jnp.pad(jnp.stack([attention_gain, feedforward_gain], axis=1), ((0, 0), (0, LANES - 2)))
    pack = jnp.concatenate([query_weight, key_matrix, value_matrix, output_weight.T, gains], axis=1)
    pack_parts = plane.fetch(pack)
    low, high = enter(me, tokens.reshape(rows_local, width), rows, chips)
    grad_low, grad_high = enter(me, cotangent.reshape(rows_local, width), rows, chips)
    sent = jnp.where(own_tensor == 0, low, high)
    cut = rows_local // 2
    pieces, others = [], []
    for index in range(2):
        pieces.append(lax.ppermute(sent[index * cut : (index + 1) * cut], "context", [(0, 1)]))
        others.append(over_tensor(pieces[index]))
    near, far = plane.join(pack_parts)
    gate_parts = plane.fetch(gate_weight)
    up_parts = plane.fetch(up_weight)
    down_parts = plane.fetch(down_weight.T)

    normed_low, normed_high, gain_rows, proj = project(low, high, near, far, query_cols + 2 * key_cols)
    attended, query, key, value, key0, value0, lse, branch, normed0_low, normed0_high = attend(
        place, proj, gain_rows, pieces, others, near, far, tables, heads, group
    )
    branch_other = over_tensor(branch)
    weights = plane.join(gate_parts) + plane.join(up_parts) + plane.join(down_parts)
    (
        hidden, gate_grad, up_grad, normed2_low, normed2_high, middle, normed2_grad, result
    ) = forward(low, high, branch, branch_other, gain_rows, grad_low, grad_high, weights)
    normed2_other = over_tensor(normed2_grad)
    result_other = over_tensor(result)

    normed2_peer = plane.to_core(normed2_high)
    gate_peer, up_peer = plane.to_core(gate_grad), plane.to_core(up_grad)
    hidden_peer, grad_peer = plane.to_core(hidden), plane.to_core(grad_high)
    gate_weight_grad = plane.scatter(weight_grad(normed2_low, normed2_peer, gate_grad, gate_peer, rows, chips))
    up_weight_grad = plane.scatter(weight_grad(normed2_low, normed2_peer, up_grad, up_peer, rows, chips))
    down_weight_grad = plane.scatter(weight_grad(grad_low, grad_peer, hidden, hidden_peer, rows, chips))
    middle_grad, branch_low, branch_high, attended_grad, gain_two = middle_back(
        normed2_grad, normed2_other, middle, gain_rows, grad_low, grad_high, near, far,
        query_cols, (query_cols + 2 * key_cols) // query_cols,
    )
    branch_peer, attended_peer = plane.to_core(branch_high), plane.to_core(attended)
    proj_cols = query_cols + 2 * key_cols
    grads, later, grads_peer = [], [], []
    for index in range(2):
        head_range = range(index * heads // 2, (index + 1) * heads // 2)
        early, grad = attend_back(place, query, key, value, key0, value0, attended_grad, lse, tables, head_range, group)
        grads.append(grad)
        later.append(lax.ppermute(early, "context", [(1, 0)]))
        grads_peer.append(plane.to_core(grad))
    output_weight_grad = plane.scatter(weight_grad(branch_low, branch_peer, attended, attended_peer, rows, chips))
    normed1_peer, normed0_peer = plane.to_core(normed_high), plane.to_core(normed0_high)
    proj_weight_grad = plane.scatter(
        proj_grad(normed_low, normed1_peer, normed0_low, normed0_peer, grads, grads_peer, rows, chips, group, proj_cols),
    )
    layer_output = leave(me, middle, result, result_other, rows, chips)
    normed1, gain_one = [], 0.0
    for index in range(2):
        part, gain_part = inputs_back(grads, later, low, high, near, far, group, proj_cols, index, 2)
        normed1.append((part, over_tensor(part)))
        gain_one = gain_one + gain_part
    gain_grads = plane.gain_grads(jnp.concatenate([gain_one, gain_two], axis=0))
    input_grad = None
    for index, (own, other) in enumerate(normed1):
        input_grad = finish(me, own, other, middle_grad, low, high, gain_rows, rows, chips, index, input_grad)
    return (
        layer_output.reshape(tokens.shape),
        input_grad.reshape(tokens.shape),
        gain_grads[0],
        proj_weight_grad[:, :query_cols],
        proj_weight_grad[:, query_cols : query_cols + key_cols],
        proj_weight_grad[:, query_cols + key_cols :],
        output_weight_grad.T,
        gain_grads[1],
        gate_weight_grad,
        up_weight_grad,
        down_weight_grad.T,
    )


def solution(mesh):
    in_specs = (
        P("shard", "context", None),
        P("shard"),
        P("shard", "tensor"),
        P("shard", "tensor"),
        P("shard", "tensor"),
        P("tensor", "shard"),
        P("shard"),
        P("shard", "tensor"),
        P("shard", "tensor"),
        P("tensor", "shard"),
        P("shard", "context", None),
    )
    out_specs = (
        P("shard", "context", None),
        P("shard", "context", None),
        P(("shard", "context")),
        P(("shard", "context"), "tensor"),
        P(("shard", "context"), "tensor"),
        P(("shard", "context"), "tensor"),
        P("tensor", ("shard", "context")),
        P(("shard", "context")),
        P(("shard", "context"), "tensor"),
        P(("shard", "context"), "tensor"),
        P("tensor", ("shard", "context")),
    )
    return jax.shard_map(shards, mesh=mesh, in_specs=in_specs, out_specs=out_specs, check_vma=False)
```
